32 devices in a mesh: seq: 16 (over z, x, core), head: 2 (over y).
Axes of the slice: x: 2, y: 2, z: 4, core: 2. Of those that a mesh axis runs over, the one named last changes fastest.
Arguments:
- queries: bfloat16 [8192, 768], P('seq', 'head'), may hold values from -7 to 7
- keys: bfloat16 [8192, 768], P('seq', 'head'), may hold values from -7 to 7
- values: bfloat16 [8192, 768], P('seq', 'head'), may hold values from -6 to 6
- w_out: bfloat16 [768, 768], P('head'), may hold values from -0.21875 to 0.21875
- d_out: bfloat16 [8192, 768], P('seq', 'head'), may hold values from -6 to 6
- slide_lengths: int32 [4], replicated, may hold values from 1 to 4096, 8192 in all
Outputs:
- out: bfloat16 [8192, 768], P('seq', 'head')
- d_queries: bfloat16 [8192, 768], P('seq', 'head')
- d_keys: bfloat16 [8192, 768], P('seq', 'head')
- d_values: bfloat16 [8192, 768], P('seq', 'head')
- d_w_out: float32 [768, 768], P('head', 'seq')
The draws below stay inside these ranges and needn't reach their ends.
Inputs may be any that keep to these rules, and one draw needn't show every extreme that they name: `slide_lengths`: the lengths sum to 8192 and the longest is exactly 4096.
All inputs are finite; a program needn't handle non-finite values.
Results may differ from the reference program's by a relative error of at most 0.012.
Values may be sent and summed in bfloat16 or wider, within the bound.
No kernel may reach another device: no remote copies, remote signals or barrier semaphores. Data moves between devices by JAX's collectives and lax.ppermute only.
A program may use at most 128 MiB of HBM per device.

```python
import math
import jax
import jax.numpy as jnp
import numpy as np
from jax import lax

D = 768
H = 16
TOK_DEV = 512
SLIDES = 4
TOKENS = 8192
LONGEST = 4096
N_SEQ = 16


def paired(key):
    base = jax.random.fold_in(key, 7)
    key_q, key_k = jax.random.split(base, 2)
    first = jnp.clip(1.4 * jax.random.normal(key_q, (TOKENS, D), jnp.float32), -5.6, 5.6)
    second = jnp.clip(1.4 * jax.random.normal(key_k, (TOKENS, D), jnp.float32), -5.6, 5.6)
    return (first, second)


def draw_queries(key, part):
    return paired(key)[0].astype(jnp.bfloat16)


def draw_keys(key, part):
    return paired(key)[1].astype(jnp.bfloat16)


def raised(drawn, key, source, target, parts, factor):
    def block_of(dim):
        return (jnp.arange(drawn.shape[dim]) // (drawn.shape[dim] // parts)).reshape((-1,) + (1,) * (drawn.ndim - 1 - dim))

    first = jax.random.permutation(key, parts)[block_of(target)]
    other_side = (block_of(target) + parts // 2) % parts
    return jnp.where((block_of(source) == first) | (block_of(source) == other_side), factor * drawn, drawn)


def block_levels(own_key, dims, shards, low, high):
    def one(position, shards_of):
        steps = jax.random.uniform(jax.random.fold_in(jax.random.fold_in(own_key, 6), position), (shards_of,), jnp.float32, low / len(shards), high / len(shards))
        return jnp.repeat(jnp.exp(steps), dims[position] // shards_of).reshape((-1,) + (1,) * (len(dims) - position - 1))

    loudness = one(*shards[0])
    for cut in shards[1:]:
        loudness = loudness * one(*cut)
    return loudness


def length_profile(number_of, total, reach, slope):
    loads = [(1 << 20) // math.isqrt(grade ** slope) + 1 for grade in range(2, number_of + 1)]
    rest, holding = total - reach - (number_of - 1), [1] * (number_of - 1)
    while rest > 0:
        movable = [i for i in range(number_of - 1) if holding[i] < reach]
        pool, remaining = sum([loads[i] for i in movable]), rest
        for i in movable:
            extra = min(reach - holding[i], max(1, remaining * loads[i] // pool), rest)
            holding[i] = holding[i] + extra
            rest = rest - extra
    return np.array([reach] + holding)


def uneven_parts(own_key, count, total, limit, skew):
    if count == 2:
        one = jax.random.randint(own_key, (), max(1, total - limit), min(limit, total - 1) + 1)
        return jnp.stack([one, total - one])
    tallies = jnp.asarray(length_profile(count, total, limit, skew), jnp.int32)
    pairs = (count - 1) // 2
    giver, sink = tallies[1:1 + 2 * pairs:2], tallies[2:2 + 2 * pairs:2]
    room = jnp.minimum(giver - 1, limit - sink)
    moved = jax.random.randint(jax.random.fold_in(own_key, 1), (pairs,), 0, 1 << 20) % (room + 1)
    tallies = tallies.at[1:1 + 2 * pairs:2].set(giver - moved).at[2:2 + 2 * pairs:2].set(sink + moved)
    return tallies[jax.random.permutation(jax.random.fold_in(own_key, 2), count)]


def normal_values(own_key, extent, scale, most, cuts=(), kind=jnp.bfloat16):
    values = jax.random.normal(own_key, extent, jnp.float32) * scale
    if len(cuts) > 0:
        values = block_levels(own_key, extent, cuts, -0.22, 0.18) * values
    return jnp.clip(values, min=-most, max=most).astype(kind)


def noise_with(key, extent, scale, reach, cuts, heavy, kind=jnp.bfloat16):
    result = scale * jax.random.normal(key, extent, jnp.float32)
    if cuts:
        result = result * block_levels(key, extent, cuts, -0.22, 0.18)
    return jnp.clip(raised(result, jax.random.fold_in(key, 3), *heavy), -reach, reach).astype(kind)


def setup_inputs(seed: int = 0) -> dict:
    streams_of = jax.random.split(jax.random.key(seed), 7)
    queries = draw_queries(jax.random.fold_in(streams_of[6], 71), 0)
    keys = draw_keys(jax.random.fold_in(streams_of[6], 71), 0)
    values = normal_values(streams_of[2], (TOKENS, D), 1.0, 6.0, ((0, 16), (1, 2)))
    w_out = normal_values(streams_of[3], (D, D), D ** -0.5, 0.21875, ((0, 2),))
    d_out = noise_with(streams_of[4], (TOKENS, D), 1.0, 6.0, ((0, 16), (1, 2)), (0, 1, 16, 2.0))
    slide_lengths = uneven_parts(streams_of[5], SLIDES, TOKENS, LONGEST, 2).astype(jnp.int32)
    return dict(queries=queries, keys=keys, values=values, w_out=w_out, d_out=d_out, slide_lengths=slide_lengths)


NEG = -1.0e30


def slide_ids(positions, starts):
    return jnp.sum((positions[..., None] >= starts).astype(jnp.int32), axis=-1).astype(jnp.int32)


def select(array, dilation, heads):
    segments = TOKENS // (TOK_DEV * dilation)
    shaped = array.reshape((segments, TOK_DEV, dilation, H) + array.shape[2:])
    return shaped[:, :, heads % dilation, heads]


def place(array, dilation, heads, fill):
    segments = array.shape[0]
    shaped = jnp.full((segments, TOK_DEV, dilation, H) + array.shape[3:], fill, array.dtype)
    shaped = shaped.at[:, :, heads % dilation, heads].set(array)
    return shaped.reshape((TOKENS, H) + array.shape[3:])


def to_bf16_f32(array):
    return lax.optimization_barrier(array.astype(jnp.bfloat16)).astype(jnp.float32)


def segment_forward(q_rows, k_rows, v_rows, row_ids, scale):
    scores = jnp.einsum("qhd,khd->hqk", q_rows.astype(jnp.float32), k_rows.astype(jnp.float32)) * scale
    allowed = row_ids.T[:, :, None] == row_ids.T[:, None, :]
    scores = jnp.where(allowed, scores, NEG)
    top = jnp.max(scores, axis=2)
    weights = jnp.exp(scores - top[:, :, None])
    total = jnp.sum(weights, axis=2)
    acc = jnp.einsum("hqk,khd->qhd", to_bf16_f32(weights), v_rows.astype(jnp.float32))
    return top.T, total.T, acc


def segment_backward(q_rows, k_rows, v_rows, d_rows, lse_rows, delta_rows, row_ids, scale):
    scores = jnp.einsum("qhd,khd->hqk", q_rows.astype(jnp.float32), k_rows.astype(jnp.float32)) * scale
    allowed = row_ids.T[:, :, None] == row_ids.T[:, None, :]
    probs = jnp.exp(jnp.where(allowed, scores, NEG) - lse_rows.T[:, :, None])
    dprob = jnp.einsum("qhd,khd->hqk", d_rows.astype(jnp.float32), v_rows.astype(jnp.float32))
    dscore = to_bf16_f32(probs * (dprob - delta_rows.T[:, :, None]) * scale)
    d_q = jnp.einsum("hqk,khd->qhd", dscore, k_rows.astype(jnp.float32))
    d_k = jnp.einsum("hqk,qhd->khd", dscore, q_rows.astype(jnp.float32))
    d_v = jnp.einsum("hqk,qhd->khd", to_bf16_f32(probs), d_rows.astype(jnp.float32))
    return d_q, d_k, d_v


def reference(queries, keys, values, w_out, d_out, slide_lengths):
    head = D // H
    scale = head ** -0.5
    starts = (jnp.cumsum(slide_lengths) - slide_lengths).astype(jnp.int32)
    heads = jnp.arange(H, dtype=jnp.int32)
    ids = slide_ids(jnp.arange(TOKENS, dtype=jnp.int32), starts)
    ids = jnp.broadcast_to(ids[:, None], (TOKENS, H))
    q3 = queries.reshape(TOKENS, H, head)
    k3 = keys.reshape(TOKENS, H, head)
    v3 = values.reshape(TOKENS, H, head)
    total_bits = N_SEQ.bit_length() - 1
    dilations = [2 ** ((level * total_bits) // 3) for level in range(4)]
    top = jnp.full((TOKENS, H), NEG, jnp.float32)
    total = jnp.zeros((TOKENS, H), jnp.float32)
    acc = jnp.zeros((TOKENS, H, head), jnp.float32)
    for dilation in dilations:
        pieces = (select(q3, dilation, heads), select(k3, dilation, heads), select(v3, dilation, heads), select(ids, dilation, heads))
        level_top, level_total, level_acc = lax.map(lambda item: segment_forward(item[0], item[1], item[2], item[3], scale), pieces)
        level_top = place(level_top, dilation, heads, NEG)
        level_total = place(level_total, dilation, heads, 0.0)
        level_acc = place(level_acc, dilation, heads, 0.0)
        newer = jnp.maximum(top, level_top)
        old_factor = jnp.exp(top - newer)
        new_factor = jnp.exp(level_top - newer)
        total = total * old_factor + level_total * new_factor
        acc = acc * old_factor[..., None] + level_acc * new_factor[..., None]
        top = newer
    attended = (acc / total[..., None]).astype(jnp.bfloat16)
    lse = top + jnp.log(total)
    flat = attended.reshape(TOKENS, D)
    out = jnp.dot(flat, w_out, preferred_element_type=jnp.float32).astype(jnp.bfloat16)
    d_att = jnp.dot(d_out, w_out.T, preferred_element_type=jnp.float32).astype(jnp.bfloat16)
    d_w_out = jnp.dot(flat.T, d_out, preferred_element_type=jnp.float32) * (TOKENS ** -0.5)
    d_att3 = d_att.reshape(TOKENS, H, head)
    delta = jnp.sum(d_att3.astype(jnp.float32) * attended.astype(jnp.float32), axis=-1)
    d_q = jnp.zeros((TOKENS, H, head), jnp.float32)
    d_k = jnp.zeros((TOKENS, H, head), jnp.float32)
    d_v = jnp.zeros((TOKENS, H, head), jnp.float32)
    for dilation in dilations:
        pieces = (select(q3, dilation, heads), select(k3, dilation, heads), select(v3, dilation, heads), select(d_att3, dilation, heads), select(lse, dilation, heads), select(delta, dilation, heads), select(ids, dilation, heads))
        grads = lax.map(lambda item: segment_backward(item[0], item[1], item[2], item[3], item[4], item[5], item[6], scale), pieces)
        d_q = d_q + place(grads[0], dilation, heads, 0.0)
        d_k = d_k + place(grads[1], dilation, heads, 0.0)
        d_v = d_v + place(grads[2], dilation, heads, 0.0)
    return (out, d_q.reshape(TOKENS, D).astype(jnp.bfloat16), d_k.reshape(TOKENS, D).astype(jnp.bfloat16), d_v.reshape(TOKENS, D).astype(jnp.bfloat16), d_w_out)
```

```python
import functools

import jax
import jax.numpy as jnp
from jax import lax
from jax.experimental import pallas as pl
from jax.experimental.pallas import tpu as pltpu
from jax.sharding import PartitionSpec as P

H = 16
PAD = 64
NEG = -1e30
BIG = 65536.0
LOG2E = 1.4426950408889634

f32 = jnp.float32
bf16 = jnp.bfloat16
i32 = jnp.int32


def iota(shape, dim):
    return lax.broadcasted_iota(i32, shape, dim)


def nn(a, b):
    return lax.dot_general(a, b, (((1,), (0,)), ((), ())), preferred_element_type=f32)


def nt(a, b):
    return lax.dot_general(a, b, (((1,), (1,)), ((), ())), preferred_element_type=f32)


def bitrev(value, bits):
    out = jnp.zeros_like(value)
    for k in range(bits):
        out = out | (((value >> k) & 1) << (bits - 1 - k))
    return out


def one_hot(hit):
    return jnp.where(hit, 1.0, 0.0).astype(bf16)


def log2_of(n):
    return n.bit_length() - 1


class Plan:
    def __init__(self, rows, width, n_seq, heads):
        self.rows, self.width, self.n_seq, self.heads = rows, width, n_seq, heads
        self.head = width // heads
        self.padded = heads * PAD
        total_bits = log2_of(n_seq)
        self.bits = [level * total_bits // 3 for level in range(4)]
        self.bmax = self.bits[3]
        self.rmax = 1 << self.bmax
        self.m0 = rows // self.rmax
        self.scale = self.head**-0.5
        self.c = self.scale * LOG2E

    def r(self, level):
        return 1 << self.bits[level]

    def n(self, level):
        return self.rows >> self.bits[level]

    def order(self, level):
        bits = list(range(self.bits[level]))
        return bits[1:] + bits[:1]

    def masks(self, level):
        out = [0]
        for bit in self.order(level):
            out = out + [m ^ (1 << bit) for m in out]
        return out

    def start(self, level, h):
        bits = self.bits[level]
        if isinstance(h, int):
            rev, v = 0, h % self.r(level)
            for k in range(bits):
                rev |= ((v >> k) & 1) << (bits - 1 - k)
            return rev * self.n(level)
        return bitrev(h & (self.r(level) - 1), bits) * self.n(level)

    def div_head(self, lane):
        mult = -(-(1 << 15) // self.head)
        return (lane * mult) >> 15

    def perm(self, g8):
        tok = iota((1, self.rows), 1)
        row = bitrev((tok & (self.rmax - 1)) ^ g8, self.bmax) * self.m0 + (tok >> self.bmax)
        return one_hot(iota((self.rows, self.rows), 0) == row)

    def row_token(self, g8):
        row = iota((1, self.rows), 1)
        lo = log2_of(self.m0)
        return ((row & (self.m0 - 1)) << self.bmax) + (bitrev(row >> lo, self.bmax) ^ g8)

    def perm_t(self, g8):
        return one_hot(iota((self.rows, self.rows), 0) == self.row_token(g8))

    def expand(self):
        f = iota((1, self.padded), 1)
        e = f & (PAD - 1)
        col = jnp.where(e < self.head, (f >> log2_of(PAD)) * self.head + e, -1)
        return one_hot(iota((self.width, self.padded), 0) == col)

    def expand_t(self):
        c = iota((1, self.width), 1)
        row = c + self.div_head(c) * (PAD - self.head)
        return one_hot(iota((self.padded, self.width), 0) == row)


def slide_bounds(lens_ref, slides):
    bounds = [jnp.int32(0)]
    for s in range(slides - 1):
        bounds.append(bounds[-1] + lens_ref[s])
    return bounds + [jnp.int32(1 << 30)]


def key_features(plan, level, dev, g8, bounds):
    r, n, lo = plan.r(level), plan.n(level), log2_of(plan.m0)
    lane = iota((1, plan.padded), 1)
    e, h = lane & (PAD - 1), lane >> log2_of(PAD)
    low = jnp.full((1, plan.padded), 1 << 30, i32)
    high = jnp.zeros((1, plan.padded), i32)
    for s in range(len(bounds) - 1):
        low = jnp.where(e == plan.head + s, bounds[s], low)
        high = jnp.where(e == plan.head + s, bounds[s + 1], high)
    if r > plan.heads:
        off = (h + g8) & (r - 1)
    else:
        off = h & (r - 1)
    low, high = low - off, high - off
    row = iota((n, 1), 0)
    rest = bitrev(row >> lo, plan.bmax - plan.bits[level]) << plan.bits[level]
    if r <= plan.heads:
        rest = rest ^ g8
    part = ((row & (plan.m0 - 1)) << plan.bmax) + rest
    pieces = []
    for mask in plan.masks(level):
        base = (dev ^ mask) * plan.rows
        hit = (part >= low - base) & (part < high - base)
        pieces.append(jnp.where(hit, 1.0, 0.0))
    return pieces[0] if len(pieces) == 1 else jnp.concatenate(pieces, axis=0)


def query_features(plan, dev, g8, bounds):
    pos = dev * plan.rows + plan.row_token(g8)
    s = iota((PAD - plan.head, plan.rows), 0)
    out = jnp.zeros((PAD - plan.head, plan.rows), f32)
    for j in range(len(bounds) - 1):
        inside = (pos >= bounds[j]) & (pos < bounds[j + 1])
        out = jnp.where(s == j, jnp.where(inside, 0.0, -BIG), out)
    return out.astype(bf16)


def where_am_i(plan):
    dev = lax.axis_index("seq")
    g8 = (lax.axis_index("head") * plan.heads) & (plan.rmax - 1)
    return dev, g8


def query_t(plan, q_ref, qt_ref, exp_t, feats):
    qt = nt(exp_t, q_ref[...])
    qt_ref[...] = qt.astype(bf16)
    for h in range(plan.heads):
        qt_ref[h * PAD + plan.head : (h + 1) * PAD, :] = feats


def prep_kernel(plan, levels, q_ref, k_ref, v_ref, *outs):
    dev, g8 = where_am_i(plan)
    perm = plan.perm(g8)
    q_out, k_out, v_out = outs[:3]
    q_out[...] = nn(perm, q_ref[...]).astype(bf16)
    kb = nn(perm, k_ref[...])
    vb = nn(perm, v_ref[...])
    k_out[...] = kb.astype(bf16)
    v_out[...] = vb.astype(bf16)
    h = plan.div_head(iota((1, plan.width), 1))
    for level, out in zip(levels, outs[3:]):
        n = plan.n(level)
        classes = min(plan.r(level), plan.heads)
        for side, full in ((0, kb), (1, vb)):
            start = plan.start(level, 0)
            pack = full[start : start + n]
            for c in range(1, classes):
                start = plan.start(level, c)
                pack = jnp.where((h & (classes - 1)) == c, full[start : start + n], pack)
            out[side] = pack.astype(bf16)


def tile_of(plan, level, h):
    n = plan.n(level)
    if level == 0:
        return 0, plan.rows, None
    start = plan.start(level, h)
    if n >= 128:
        return pl.multiple_of(start, 128), n, None
    first = pl.multiple_of((start >> 7) << 7, 128)
    lane = iota((1, 128), 1) + first
    return first, 128, (lane >= start) & (lane < start + n)


def forward_kernel(plan, levels, init, last, slides, *refs):
    refs = list(refs)
    lens_ref, q_ref = refs[:2]
    kv = refs[2 : 2 + 2 * len(levels)]
    refs = refs[2 + 2 * len(levels) :]
    if not init:
        acc_in, top_in = refs[:2]
        refs = refs[2:]
    if last:
        do_ref, w_ref, d_mine, d_other = refs[:4]
        att_out, send_out, own_out, dw_out, lse_out, delta_out = refs[4:10]
        refs = refs[10:]
        acc_ref, top_ref, qt_ref, kp_ref, vt_ref, at_ref = refs
    else:
        acc_ref, top_ref, qt_ref, kp_ref, vt_ref = refs
    dev, g8 = where_am_i(plan)
    bounds = slide_bounds(lens_ref, slides)
    exp, exp_t = plan.expand(), plan.expand_t()
    query_t(plan, q_ref, qt_ref, exp_t, query_features(plan, dev, g8, bounds))
    if not init:
        acc_ref[...] = acc_in[...]
        top_ref[...] = top_in[...]
    ones = jnp.where((iota((plan.padded, 1), 0) & (PAD - 1)) == plan.head, 1.0, 0.0)
    zeros = jnp.zeros((PAD, plan.rows), bf16)
    for index, level in enumerate(levels):
        k, v = kv[2 * index][...], kv[2 * index + 1][...]
        kp_ref[...] = (nn(k, exp) + key_features(plan, level, dev, g8, bounds)).astype(bf16)
        vt_ref[...] = (nt(exp_t, v) + ones).astype(bf16)

        def pair(j, _):
            lanes = pl.ds(pl.multiple_of(j * 2 * PAD, 2 * PAD), 2 * PAD)
            kp = kp_ref[:, lanes]
            for side in range(2):
                h = 2 * j + side
                feats = pl.ds(pl.multiple_of(h * PAD, PAD), PAD)
                first, w, inside = tile_of(plan, level, h)
                cols = pl.ds(first, w)
                q = qt_ref[feats, cols]
                z = zeros[:, :w]
                q = jnp.concatenate([q, z] if side == 0 else [z, q], axis=0)
                scores = nn(kp, q)
                top = jnp.max(scores, axis=0, keepdims=True)
                weights = jnp.exp2((scores - top) * plan.c)
                acc = nn(vt_ref[feats, :], weights.astype(bf16))
                top = top * plan.c
                if level == 0:
                    acc_ref[feats, cols] = acc
                    top_ref[h, :, cols] = top
                else:
                    if inside is not None:
                        top = jnp.where(inside, top, NEG)
                    old = top_ref[h, :, cols]
                    new = jnp.maximum(old, top)
                    acc_ref[feats, cols] = acc_ref[feats, cols] * jnp.exp2(old - new) + acc * jnp.exp2(top - new)
                    top_ref[h, :, cols] = new
            return 0

        lax.fori_loop(0, plan.heads // 2, pair, 0)
    if last:
        dot = nt(exp_t, do_ref[...])
        for h in range(plan.heads):
            lo = h * PAD
            total = acc_ref[lo + plan.head : lo + plan.head + 1, :]
            att = (acc_ref[lo : lo + PAD, :] * (1.0 / total)).astype(bf16)
            at_ref[lo : lo + PAD, :] = att
            lse_out[h] = top_ref[h] + jnp.log2(total)
            delta_out[h] = jnp.sum(att.astype(f32) * dot[lo : lo + PAD, :], axis=0, keepdims=True)
        compact = nn(exp, at_ref[...]).astype(bf16)
        perm_t = plan.perm_t(g8)
        att = nt(perm_t, compact).astype(bf16)
        att_t = nn(compact, plan.perm(g8)).astype(bf16)
        att_out[...] = att
        group = lax.axis_index("head")
        full = nn(att, w_ref[...])
        left, right = full[:, : plan.width], full[:, plan.width :]
        own_out[...] = jnp.where(group == 0, left, right)
        send_out[...] = jnp.where(group == 0, right, left).astype(bf16)
        mine, other = nn(att_t, d_mine[...]), nn(att_t, d_other[...])
        dw_out[:, : plan.width] = jnp.where(group == 0, mine, other).astype(bf16)
        dw_out[:, plan.width :] = jnp.where(group == 0, other, mine).astype(bf16)


def cotangent_kernel(plan, d_mine, d_other, w_ref, out):
    _, g8 = where_am_i(plan)
    group = lax.axis_index("head")
    mine, other = d_mine[...], d_other[...]
    left = jnp.where(group == 0, mine, other)
    right = jnp.where(group == 0, other, mine)
    d = nt(left, w_ref[:, : plan.width]) + nt(right, w_ref[:, plan.width :])
    out[...] = nn(plan.perm(g8), d.astype(bf16)).astype(bf16)


def backward_kernel(plan, levels, init, last, slides, *refs):
    refs = list(refs)
    lens_ref, q_ref, do_ref, lse_ref, delta_ref = refs[:5]
    kv = refs[5 : 5 + 2 * len(levels)]
    refs = refs[5 + 2 * len(levels) :]
    if not init:
        dq_in = refs.pop(0)
    grads = refs[: len(levels)]
    refs = refs[len(levels) :]
    if last:
        dq_final = refs.pop(0)
    dq_ref, qt_ref, qp_ref, dot_ref, dop_ref, kp_ref, kt_ref, vp_ref, dk_ref, dv_ref = refs
    dev, g8 = where_am_i(plan)
    bounds = slide_bounds(lens_ref, slides)
    exp, exp_t = plan.expand(), plan.expand_t()
    query_t(plan, q_ref, qt_ref, exp_t, query_features(plan, dev, g8, bounds))
    qp_ref[...] = nn(q_ref[...], exp).astype(bf16)
    dot_ref[...] = nt(exp_t, do_ref[...]).astype(bf16)
    dop_ref[...] = nn(do_ref[...], exp).astype(bf16)
    if init:
        dq_ref[...] = jnp.zeros_like(dq_ref)
    else:
        dq_ref[...] = dq_in[...]
    zeros = jnp.zeros((PAD, plan.rows), bf16)
    lower = iota((plan.rows, 2 * PAD), 1) < PAD
    for index, level in enumerate(levels):
        k, v = kv[2 * index][...], kv[2 * index + 1][...]
        kp_ref[...] = (nn(k, exp) + key_features(plan, level, dev, g8, bounds)).astype(bf16)
        kt_ref[...] = nt(exp_t, k).astype(bf16)
        vp_ref[...] = nn(v, exp).astype(bf16)

        def pair(j, _):
            lanes = pl.ds(pl.multiple_of(j * 2 * PAD, 2 * PAD), 2 * PAD)
            kp, vp = kp_ref[:, lanes], vp_ref[:, lanes]
            dks, dvs = [], []
            for side in range(2):
                h = 2 * j + side
                feats = pl.ds(pl.multiple_of(h * PAD, PAD), PAD)
                first, w, inside = tile_of(plan, level, h)
                cols = pl.ds(first, w)
                z = zeros[:, :w]
                q, do = qt_ref[feats, cols], dot_ref[feats, cols]
                q = jnp.concatenate([q, z] if side == 0 else [z, q], axis=0)
                do = jnp.concatenate([do, z] if side == 0 else [z, do], axis=0)
                lse = lse_ref[h, :, cols]
                if inside is not None:
                    lse = jnp.where(inside, lse, -NEG)
                probs = jnp.exp2(nn(kp, q) * plan.c - lse)
                dscore = (probs * (nn(vp, do) - delta_ref[h, :, cols])).astype(bf16)
                dvs.append(nn(probs.astype(bf16), dop_ref[cols, lanes]))
                dks.append(nn(dscore, qp_ref[cols, lanes]))
                dq_ref[feats, cols] = dq_ref[feats, cols] + nn(kt_ref[feats, :], dscore)
            dk_ref[:, lanes] = (jnp.where(lower, dks[0], dks[1]) * plan.scale).astype(bf16)
            dv_ref[:, lanes] = jnp.where(lower, dvs[0], dvs[1]).astype(bf16)
            return 0

        lax.fori_loop(0, plan.heads // 2, pair, 0)
        grads[index][0] = nn(dk_ref[...], exp_t).astype(bf16)
        grads[index][1] = nn(dv_ref[...], exp_t).astype(bf16)
    if last:
        compact = nn(exp, (dq_ref[...] * plan.scale).astype(bf16)).astype(bf16)
        dq_final[...] = nt(plan.perm_t(g8), compact).astype(bf16)


def final_kernel(plan, levels, *refs):
    refs = list(refs)
    own = refs.pop(0)
    packs = refs[: 2 * len(levels)]
    out_own, out_came, out_ref, dk_ref, dv_ref = refs[2 * len(levels) :]
    _, g8 = where_am_i(plan)
    perm_t = plan.perm_t(g8)
    h = plan.div_head(iota((1, plan.width), 1))
    for side, ref in ((0, dk_ref), (1, dv_ref)):
        total = own[side].astype(f32)
        for index, level in enumerate(levels):
            n = plan.n(level)
            classes = min(plan.r(level), plan.heads)
            pack = packs[2 * index][side].astype(f32) + packs[2 * index + 1][side].astype(f32)
            at = {plan.start(level, c): c for c in range(classes)}
            pieces = []
            for start in range(0, plan.rows, n):
                if start in at:
                    pieces.append(jnp.where((h & (classes - 1)) == at[start], pack, 0.0))
                else:
                    pieces.append(jnp.zeros((n, plan.width), f32))
            total = total + jnp.concatenate(pieces, axis=0)
        ref[...] = nn(perm_t, total.astype(bf16)).astype(bf16)
    out_ref[...] = (out_own[...] + out_came[...].astype(f32)).astype(bf16)


def swapped(block, axis, mask):
    count = lax.axis_size(axis)
    return lax.ppermute(block, axis, [(i, i ^ mask) for i in range(count)])


def shape(dims, dtype):
    return jax.ShapeDtypeStruct(dims, dtype)


def vmem(count):
    return [pl.BlockSpec(memory_space=pltpu.VMEM)] * count


def run(body, name, ins, outs, scratch=(), smem=0, flops=0):
    return pl.pallas_call(
        body,
        name=name,
        out_shape=outs,
        in_specs=[pl.BlockSpec(memory_space=pltpu.SMEM)] * smem + vmem(len(ins) - smem),
        out_specs=vmem(len(outs)),
        scratch_shapes=list(scratch),
        compiler_params=pltpu.CompilerParams(vmem_limit_bytes=48 * 1024 * 1024),
        cost_estimate=pl.CostEstimate(flops=flops, bytes_accessed=4 << 20, transcendentals=0),
    )(*ins)


def shards(queries, keys, values, w_out, d_out, slide_lengths):
    rows, width = queries.shape
    n_seq = lax.axis_size("seq")
    heads = H // lax.axis_size("head")
    slides = slide_lengths.shape[0]
    plan = Plan(rows, width, n_seq, heads)
    padded = plan.padded
    levels = [level for level in range(1, 4) if plan.bits[level] > 0]
    part = functools.partial

    def mat(a, b, dtype=bf16):
        return pltpu.VMEM((a, b), dtype)

    d_other = swapped(d_out, "head", 1)
    compact = shape((rows, width), bf16)
    prepared = run(
        part(prep_kernel, plan, levels),
        "prep",
        (queries, keys, values),
        [compact] * 3 + [shape((2, plan.n(level), width), bf16) for level in levels],
        flops=10**9,
    )
    q_br, k_br, v_br = prepared[:3]
    gathered = {0: (k_br, v_br)}
    for level, pack in zip(levels, prepared[3:]):
        for bit in plan.order(level):
            pack = jnp.concatenate([pack, swapped(pack, "seq", 1 << bit)], axis=1)
        gathered[level] = (pack[0], pack[1])

    state = [shape((padded, rows), f32), shape((heads, 1, rows), f32)]
    square = mat(padded, rows)
    fwd_scratch = [square, mat(rows, padded), square]

    def kv_of(chosen):
        return sum((gathered[level] for level in chosen), ())

    acc, top = run(
        part(forward_kernel, plan, [0], True, False, slides),
        "fwd0",
        (slide_lengths, q_br) + kv_of([0]),
        state,
        fwd_scratch,
        smem=1,
        flops=3 * 10**9,
    )
    d_att = run(
        part(cotangent_kernel, plan),
        "cot",
        (d_out, d_other, w_out),
        [compact],
        flops=10**9,
    )[0]
    model = w_out.shape[1]
    _, out_send, out_own, dw, lse, delta = run(
        part(forward_kernel, plan, levels, False, True, slides),
        "fwd1",
        (slide_lengths, q_br) + kv_of(levels) + (acc, top, d_att, w_out, d_out, d_other),
        [compact, compact, shape((rows, width), f32), shape((width, model), bf16)]
        + [shape((heads, 1, rows), f32)] * 2,
        [mat(padded, rows, f32), pltpu.VMEM((heads, 1, rows), f32)] + fwd_scratch + [square],
        smem=1,
        flops=3 * 10**9,
    )
    out_came = swapped(out_send, "head", 1)

    device = lax.axis_index("seq")
    total_bits = log2_of(n_seq)
    block = dw.reshape((width,) + (2,) * total_bits + (model // n_seq,))
    axis_bits = [total_bits - 1 - a for a in range(total_bits)]
    for bit in range(total_bits):
        axis = axis_bits.index(bit) + 1
        mine = device >> bit & 1
        keep = lax.dynamic_index_in_dim(block, mine, axis, keepdims=False)
        send = lax.dynamic_index_in_dim(block, 1 - mine, axis, keepdims=False)
        came = swapped(send.astype(bf16), "seq", 1 << bit)
        block = keep.astype(f32) + came.astype(f32)
        axis_bits.pop(axis - 1)
    d_w_out = block * (rows * n_seq) ** -0.5

    bwd_scratch = [square, mat(rows, padded)] * 2 + [mat(rows, padded), square] + [mat(rows, padded)] * 3
    base = (slide_lengths, q_br, d_att, lse, delta)
    grad = shape((2, rows, width), bf16)
    dq_state = shape((padded, rows), f32)
    back = levels[::-1]
    *grads, dq = run(
        part(backward_kernel, plan, back, True, False, slides),
        "bwd1",
        base + kv_of(back),
        [grad] * len(back) + [dq_state],
        bwd_scratch,
        smem=1,
        flops=4 * 10**9,
    )
    dkv0, d_q = run(
        part(backward_kernel, plan, [0], False, True, slides),
        "bwd0",
        base + kv_of([0]) + (dq,),
        [grad, compact],
        [mat(padded, rows, f32)] + bwd_scratch,
        smem=1,
        flops=6 * 10**9,
    )
    packs = []
    by_level = dict(zip(back, grads))
    for level in levels:
        pack = by_level[level]
        order = plan.order(level)[::-1]
        for step, bit in enumerate(order):
            half = pack.shape[1] // 2
            keep = pack[:, :half]
            came = swapped(pack[:, half:], "seq", 1 << bit)
            if step == len(order) - 1:
                packs += [keep, came]
            else:
                pack = (keep.astype(f32) + came.astype(f32)).astype(bf16)
    out, d_k, d_v = run(
        part(final_kernel, plan, levels),
        "final",
        (dkv0, *packs, out_own, out_came),
        [compact] * 3,
        flops=10**9,
    )
    return out, d_q, d_k, d_v, d_w_out


def solution(mesh):
    in_specs = (
        P("seq", "head"),
        P("seq", "head"),
        P("seq", "head"),
        P("head", None),
        P("seq", "head"),
        P(),
    )
    out_specs = (
        P("seq", "head"),
        P("seq", "head"),
        P("seq", "head"),
        P("seq", "head"),
        P("head", "seq"),
    )
    return jax.shard_map(shards, mesh=mesh, in_specs=in_specs, out_specs=out_specs, check_vma=False)
```
